8 devices in a mesh: tasks: 1 (over z), group: 8 (over y, x, core).
Axes of the slice: x: 2, y: 2, z: 1, core: 2. Of those that a mesh axis runs over, the one named last changes fastest.
Arguments:
- points: bfloat16 [16384, 512], P(('tasks', 'group'))
- vectors: bfloat16 [16384, 128], P(('tasks', 'group'))
- lengthscale: float32 [1], replicated
- outscale: float32 [1], replicated
Outputs:
- output: float32 [16384, 128], P(('tasks', 'group'))
All inputs are finite; a program needn't handle non-finite values.
Results may differ from the reference program's by a relative error of at most 0.001.
Values are sent between devices in bfloat16 or wider.
A program may use at most 1 GiB of HBM per device.

```python
import jax
import jax.numpy as jnp
from jax import lax

NUM_POINTS = 16384
FEAT_DIM = 512
NUM_RHS = 128
QUERY_BLOCK = 256
LATENT_DIM = 8


def setup_inputs(seed: int = 0, part: int = 0) -> dict:
    base_key = jax.random.key(seed)
    part_key = jax.random.fold_in(base_key, part)
    key_lat, key_mix, key_noise, key_rhs = jax.random.split(part_key, 4)
    key_ell, key_scale = jax.random.split(jax.random.key(seed + 29), 2)
    latent = jax.random.normal(key_lat, (NUM_POINTS, LATENT_DIM), jnp.float32)
    mixing = jax.random.normal(key_mix, (LATENT_DIM, FEAT_DIM), jnp.float32) * FEAT_DIM ** -0.5
    noise = jax.random.normal(key_noise, (NUM_POINTS, FEAT_DIM), jnp.float32) * (0.3 * FEAT_DIM ** -0.5)
    points = (jnp.dot(latent, mixing) + noise).astype(jnp.bfloat16)
    vectors = (jax.random.normal(key_rhs, (NUM_POINTS, NUM_RHS), jnp.float32) * NUM_POINTS ** -0.5).astype(jnp.bfloat16)
    lengthscale = jax.random.uniform(key_ell, (1,), jnp.float32, 2.4, 3.1)
    outscale = jax.random.uniform(key_scale, (1,), jnp.float32, 0.6, 1.6)
    return {'points': points, 'vectors': vectors, 'lengthscale': lengthscale, 'outscale': outscale}


def reference(points, vectors, lengthscale, outscale):
    sq_norm = jnp.sum(jnp.square(points.astype(jnp.float32)), axis=1)
    two_ell_sq = 2.0 * jnp.square(lengthscale[0])
    query_pts = points.reshape(NUM_POINTS // QUERY_BLOCK, QUERY_BLOCK, FEAT_DIM)
    query_norm = sq_norm.reshape(NUM_POINTS // QUERY_BLOCK, QUERY_BLOCK)

    def one_block(block_pair):
        block_pts, block_norm = block_pair
        gram_mat = jnp.dot(block_pts, points.T, preferred_element_type=jnp.float32)
        sq_dist = jnp.maximum(block_norm[:, None] + sq_norm[None, :] - 2.0 * gram_mat, 0.0)
        kern_blk = (outscale[0] * jnp.exp(-sq_dist / two_ell_sq)).astype(jnp.bfloat16)
        return jnp.dot(kern_blk, vectors, preferred_element_type=jnp.float32)

    result = lax.map(one_block, (query_pts, query_norm))
    return result.reshape(NUM_POINTS, NUM_RHS)
```

```python
import functools

import jax
import jax.numpy as jnp
from jax import lax
from jax.experimental import pallas as pl
from jax.experimental.pallas import tpu as pltpu
from jax.sharding import PartitionSpec as P

ROWS = 2048
HALF = ROWS // 2
CHUNK = 512
N_CHUNK = ROWS // CHUNK
SUB = 256
FEAT = 512
RHS = 128
LOG2E = 1.4426950408889634
OWN, PAIR = 0, 1
X_ROWS, Y_ROWS = ROWS, ROWS + HALF


def local_kernel(x_hbm, v_hbm, ell_ref, scale_ref, out_ref,
                 x_all, v_all, lhs, norm_lhs, acc, back, consts,
                 load_sem, pair_send, pair_recv, link_send, link_recv,
                 fwd_send, fwd_recv, back_send, back_recv):
    me = lax.axis_index('group')
    core = lax.rem(me, 2)
    chip_x = lax.rem(me // 2, 2)
    chip_y = me // 4
    pair = me + 1 - 2 * core
    neighbour = (me + 2 - 4 * chip_x, me + 4 - 8 * chip_y)

    load_x = pltpu.make_async_copy(x_hbm, x_all.at[pl.ds(0, ROWS)], load_sem.at[0])
    load_v = pltpu.make_async_copy(v_hbm, v_all.at[pl.ds(0, ROWS)], load_sem.at[1])
    load_x.start()
    load_v.start()

    barrier = pltpu.get_barrier_semaphore()
    for peer in (pair,) + neighbour:
        pl.semaphore_signal(barrier, inc=1, device_id={'group': peer}, device_id_type=pl.DeviceIdType.MESH)
    pl.semaphore_wait(barrier, 3)

    def remote(src, dst, send, recv, peer):
        return pltpu.make_async_remote_copy(src_ref=src, dst_ref=dst, send_sem=send, recv_sem=recv,
                                            device_id={'group': peer}, device_id_type=pl.DeviceIdType.MESH)

    def rows_of(block, chunk):
        return pl.ds(pl.multiple_of(block * ROWS + chunk * CHUNK, CHUNK), CHUNK)

    def pair_copies():
        return (remote(x_all.at[pl.ds(0, ROWS)], x_all.at[pl.ds(PAIR * ROWS, ROWS)], pair_send.at[0], pair_recv.at[0], pair),
                remote(v_all.at[pl.ds(0, ROWS)], v_all.at[pl.ds(PAIR * ROWS, ROWS)], pair_send.at[1], pair_recv.at[1], pair))

    def link_copies(axis, chunk):
        src, dst = rows_of(OWN, chunk), rows_of(2 + 2 * axis, chunk)
        return (remote(x_all.at[src], x_all.at[dst], link_send.at[0, axis, chunk], link_recv.at[0, axis, chunk], neighbour[axis]),
                remote(v_all.at[src], v_all.at[dst], link_send.at[1, axis, chunk], link_recv.at[1, axis, chunk], neighbour[axis]))

    def fwd_copies(axis, chunk):
        src, dst = rows_of(2 + 2 * axis, chunk), rows_of(3 + 2 * axis, chunk)
        return (remote(x_all.at[src], x_all.at[dst], fwd_send.at[0, axis, chunk], fwd_recv.at[0, axis, chunk], pair),
                remote(v_all.at[src], v_all.at[dst], fwd_send.at[1, axis, chunk], fwd_recv.at[1, axis, chunk], pair))

    def back_copy(axis):
        return remote(acc.at[pl.ds(ROWS + axis * HALF, HALF)], back.at[pl.ds(axis * HALF, HALF)],
                      back_send.at[axis], back_recv.at[axis], neighbour[axis])

    def chunk_of(axis, step):
        return lax.rem(step + 2 * axis, N_CHUNK)

    load_x.wait()
    load_v.wait()
    for step in range(N_CHUNK):
        for axis in (0, 1):
            for copy in link_copies(axis, (step + 2 * axis) % N_CHUNK):
                copy.start()
        if step == 0:
            for copy in pair_copies():
                copy.start()

    ell = jnp.full((8, 128), ell_ref[0], jnp.float32)
    consts[0] = -LOG2E / (2.0 * (ell * ell))
    consts[1] = jnp.full((8, 128), scale_ref[0], jnp.float32)

    def set_rows(source, target, count):
        @pl.loop(0, count // CHUNK)
        def _(part):
            rows = x_all[pl.ds(pl.multiple_of(source + part * CHUNK, CHUNK), CHUNK), :]
            at = pl.ds(pl.multiple_of(target + part * CHUNK, CHUNK), CHUNK)
            lhs[at, :] = rows * jnp.bfloat16(-2)
            wide = rows.astype(jnp.float32)
            norm_lhs[at, :] = jnp.broadcast_to(jnp.sum(wide * wide, axis=1, keepdims=True), (CHUNK, 128))
            acc[at, :] = jnp.zeros((CHUNK, RHS), jnp.float32)

    def add_columns(row_start, row_count, cols):
        x_col = x_all[cols, :]
        v_col = v_all[cols, :]
        wide = x_col.astype(jnp.float32)
        norm_col = jnp.broadcast_to(jnp.sum(wide * wide, axis=1, keepdims=True), (CHUNK, 128)).T[0:1, :]
        rate = jnp.concatenate([consts[0, 0:1, :]] * (CHUNK // 128), axis=1)
        scale = jnp.concatenate([consts[1, 0:1, :]] * (CHUNK // 128), axis=1)
        parts = [pl.ds(pl.multiple_of(row_start + i * SUB, SUB), SUB) for i in range(row_count // SUB)]
        grams = [lax.dot_general(lhs[rows, :], x_col, (((1,), (1,)), ((), ())), preferred_element_type=jnp.float32)
                 for rows in parts]
        for rows, gram in zip(parts, grams):
            norm_row = jnp.concatenate([norm_lhs[rows, :]] * (CHUNK // 128), axis=1)
            dist = jnp.maximum((norm_row + norm_col) + gram, 0.0)
            kern = (scale * jnp.exp2(dist * rate)).astype(jnp.bfloat16)
            acc[rows, :] += jnp.dot(kern, v_col, preferred_element_type=jnp.float32)

    def block_of(q):
        return 2 + 2 * lax.rem(q, 2) + q // 2

    def cols_of(step, q):
        return rows_of(block_of(q), lax.rem(step + 2 * lax.rem(q, 2), N_CHUNK))

    def receive(step):
        for axis in (0, 1):
            chunk = chunk_of(axis, step)
            for copy in link_copies(axis, chunk):
                copy.wait_recv()
            for copy in fwd_copies(axis, chunk):
                copy.start()

    def receive_forwarded(step):
        for axis in (0, 1):
            for copy in fwd_copies(axis, chunk_of(axis, step)):
                copy.wait_recv()

    def far_columns(step, q):
        add_columns(jnp.where(lax.rem(q, 2) == 0, Y_ROWS, X_ROWS), HALF, cols_of(step, q))

    set_rows(0, 0, ROWS)

    @pl.loop(0, 2 * N_CHUNK)
    def _(c):
        @pl.when(c == N_CHUNK)
        def _():
            for copy in pair_copies():
                copy.wait_recv()
        add_columns(0, ROWS, rows_of(0, c))

    @pl.loop(0, N_CHUNK // 2)
    def _(step):
        receive(step)

        @pl.loop(0, 4)
        def _(q):
            @pl.when(q == 2)
            def _():
                receive_forwarded(step)
            add_columns(0, ROWS, cols_of(step, q))

    set_rows(2 * ROWS, X_ROWS, HALF)
    set_rows(4 * ROWS + HALF, Y_ROWS, HALF)

    @pl.loop(0, N_CHUNK // 2)
    def _(step):
        @pl.loop(0, 4)
        def _(q):
            far_columns(step, q)

    @pl.loop(N_CHUNK // 2, N_CHUNK)
    def _(step):
        receive(step)

        @pl.loop(0, 4)
        def _(q):
            @pl.when(q == 2)
            def _():
                receive_forwarded(step)
            far_columns(step, q)

        @pl.when(step == N_CHUNK - 1)
        def _():
            for axis in (0, 1):
                back_copy(axis).start()

        @pl.loop(0, 4)
        def _(q):
            add_columns(0, ROWS, cols_of(step, q))

    for axis in (0, 1):
        back_copy(axis).wait_recv()
    out_ref[...] = acc[pl.ds(0, ROWS), :] + back[...]

    for copy in pair_copies():
        copy.wait_send()
    for axis in (0, 1):
        back_copy(axis).wait_send()
        for chunk in range(N_CHUNK):
            for copy in link_copies(axis, chunk) + fwd_copies(axis, chunk):
                copy.wait_send()


def solution(mesh):
    row_spec = P(('tasks', 'group'), None)
    dma = pltpu.SemaphoreType.DMA

    def local_fn(x_loc, v_loc, lengthscale, outscale):
        return pl.pallas_call(
            local_kernel,
            out_shape=jax.ShapeDtypeStruct((ROWS, RHS), jnp.float32),
            in_specs=[pl.BlockSpec(memory_space=pl.ANY), pl.BlockSpec(memory_space=pl.ANY),
                      pl.BlockSpec(memory_space=pltpu.SMEM), pl.BlockSpec(memory_space=pltpu.SMEM)],
            out_specs=pl.BlockSpec(memory_space=pltpu.VMEM),
            scratch_shapes=[
                pltpu.VMEM((6 * ROWS, FEAT), jnp.bfloat16),
                pltpu.VMEM((6 * ROWS, RHS), jnp.bfloat16),
                pltpu.VMEM((2 * ROWS, FEAT), jnp.bfloat16),
                pltpu.VMEM((2 * ROWS, 128), jnp.float32),
                pltpu.VMEM((2 * ROWS, RHS), jnp.float32),
                pltpu.VMEM((ROWS, RHS), jnp.float32),
                pltpu.VMEM((2, 8, 128), jnp.float32),
                dma((2,)), dma((2,)), dma((2,)),
                dma((2, 2, N_CHUNK)), dma((2, 2, N_CHUNK)),
                dma((2, 2, N_CHUNK)), dma((2, 2, N_CHUNK)),
                dma((2,)), dma((2,)),
            ],
            compiler_params=pltpu.CompilerParams(collective_id=0, has_side_effects=True, vmem_limit_bytes=60 * 2 ** 20),
        )(x_loc, v_loc, lengthscale, outscale)

    return jax.shard_map(local_fn, mesh=mesh, in_specs=(row_spec, row_spec, P(None), P(None)), out_specs=row_spec, check_vma=False)
```

```python
import functools

import jax
import jax.numpy as jnp
from jax import lax
from jax.experimental import pallas as pl
from jax.experimental.pallas import tpu as pltpu
from jax.sharding import PartitionSpec as P

ROWS = 2048
HALF = ROWS // 2
CHUNK = 512
PIECE = 256
N_CHUNK = ROWS // CHUNK
N_PIECE = ROWS // PIECE
SUB = 256
FEAT = 512
RHS = 128
LOG2E = 1.4426950408889634
OWN, PAIR = 0, 1
X_ROWS, Y_ROWS = ROWS, ROWS + HALF


def local_kernel(x_hbm, v_hbm, ell_ref, scale_ref, out_ref,
                 x_all, v_all, lhs, norm_lhs, acc, back,
                 load_sem, pair_send, pair_recv, link_send, link_recv,
                 fwd_send, fwd_recv, back_send, back_recv):
    me = lax.axis_index('group')
    core = lax.rem(me, 2)
    chip_x = lax.rem(me // 2, 2)
    chip_y = me // 4
    pair = me + 1 - 2 * core
    neighbour = (me + 2 - 4 * chip_x, me + 4 - 8 * chip_y)

    load_x = pltpu.make_async_copy(x_hbm, x_all.at[pl.ds(0, ROWS)], load_sem.at[0])
    load_v = pltpu.make_async_copy(v_hbm, v_all.at[pl.ds(0, ROWS)], load_sem.at[1])
    load_x.start()
    load_v.start()

    barrier = pltpu.get_barrier_semaphore()
    for peer in (pair,) + neighbour:
        pl.semaphore_signal(barrier, inc=1, device_id={'group': peer}, device_id_type=pl.DeviceIdType.MESH)
    pl.semaphore_wait(barrier, 3)

    def remote(src, dst, send, recv, peer):
        return pltpu.make_async_remote_copy(src_ref=src, dst_ref=dst, send_sem=send, recv_sem=recv,
                                            device_id={'group': peer}, device_id_type=pl.DeviceIdType.MESH)

    def rows_of(block, chunk):
        return pl.ds(pl.multiple_of(block * ROWS + chunk * CHUNK, CHUNK), CHUNK)

    def piece_of(block, piece):
        return pl.ds(pl.multiple_of(block * ROWS + piece * PIECE, PIECE), PIECE)

    def pair_copies():
        return (remote(x_all.at[pl.ds(0, ROWS)], x_all.at[pl.ds(PAIR * ROWS, ROWS)], pair_send.at[0], pair_recv.at[0], pair),
                remote(v_all.at[pl.ds(0, ROWS)], v_all.at[pl.ds(PAIR * ROWS, ROWS)], pair_send.at[1], pair_recv.at[1], pair))

    def link_copies(axis, piece):
        src, dst = piece_of(OWN, piece), piece_of(2 + 2 * axis, piece)
        return (remote(x_all.at[src], x_all.at[dst], link_send.at[0, axis, piece], link_recv.at[0, axis, piece], neighbour[axis]),
                remote(v_all.at[src], v_all.at[dst], link_send.at[1, axis, piece], link_recv.at[1, axis, piece], neighbour[axis]))

    def fwd_copies(axis, piece):
        src, dst = piece_of(2 + 2 * axis, piece), piece_of(3 + 2 * axis, piece)
        return (remote(x_all.at[src], x_all.at[dst], fwd_send.at[0, axis, piece], fwd_recv.at[0, axis, piece], pair),
                remote(v_all.at[src], v_all.at[dst], fwd_send.at[1, axis, piece], fwd_recv.at[1, axis, piece], pair))

    def back_copy(axis):
        return remote(acc.at[pl.ds(ROWS + axis * HALF, HALF)], back.at[pl.ds(axis * HALF, HALF)],
                      back_send.at[axis], back_recv.at[axis], neighbour[axis])

    def chunk_of(axis, step):
        return lax.rem(step + 2 * axis, N_CHUNK)

    def piece_at(axis, step):
        return lax.rem(step + (N_PIECE // 2) * axis, N_PIECE)

    load_x.wait()
    load_v.wait()
    for step in range(N_PIECE):
        for axis in (0, 1):
            for copy in link_copies(axis, (step + N_PIECE // 2 * axis) % N_PIECE):
                copy.start()
        if step == 0:
            for copy in pair_copies():
                copy.start()

    ell = jnp.full((8, 128), ell_ref[0], jnp.float32)
    rate = (-LOG2E / (2.0 * (ell * ell)))[0, 0]
    scale = scale_ref[0]

    def set_rows(source, target, count):
        @pl.loop(0, count // CHUNK)
        def _(part):
            rows = x_all[pl.ds(pl.multiple_of(source + part * CHUNK, CHUNK), CHUNK), :]
            at = pl.ds(pl.multiple_of(target + part * CHUNK, CHUNK), CHUNK)
            lhs[at, :] = rows * jnp.bfloat16(-2)
            wide = rows.astype(jnp.float32)
            norm_lhs[at, :] = jnp.broadcast_to(jnp.sum(wide * wide, axis=1, keepdims=True), (CHUNK, 128))
            acc[at, :] = jnp.zeros((CHUNK, RHS), jnp.float32)

    def add_columns(items, row_count, width, same_rows):
        work = []
        for row_start, cols in items:
            x_col = x_all[cols, :]
            wide = x_col.astype(jnp.float32)
            norm_col = jnp.broadcast_to(jnp.sum(wide * wide, axis=1, keepdims=True), (width, 128)).T[0:1, :]
            for i in range(row_count // SUB):
                rows = pl.ds(pl.multiple_of(row_start + i * SUB, SUB), SUB)
                gram = lax.dot_general(lhs[rows, :], x_col, (((1,), (1,)), ((), ())), preferred_element_type=jnp.float32)
                work.append((rows, cols, norm_col, gram))
        def part_sum(rows, cols, norm_col, gram):
            norm_row = jnp.concatenate([norm_lhs[rows, :]] * (width // 128), axis=1)
            dist = jnp.maximum((norm_row + norm_col) + gram, 0.0)
            kern = (scale * jnp.exp2(dist * rate)).astype(jnp.bfloat16)
            return jnp.dot(kern, v_all[cols, :], preferred_element_type=jnp.float32)
        per_item = row_count // SUB
        if same_rows:
            for i in range(per_item):
                acc[work[i][0], :] += part_sum(*work[i]) + part_sum(*work[per_item + i])
        else:
            for one in work:
                acc[one[0], :] += part_sum(*one)

    def cols_of(axis, forwarded, step):
        return rows_of(2 + 2 * axis + forwarded, chunk_of(axis, step))

    def receive(step):
        for axis in (0, 1):
            piece = piece_at(axis, step)
            for copy in link_copies(axis, piece):
                copy.wait_recv()
            for copy in fwd_copies(axis, piece):
                copy.start()

    def receive_forwarded(step):
        for axis in (0, 1):
            for copy in fwd_copies(axis, piece_at(axis, step)):
                copy.wait_recv()

    def own_columns(step, forwarded):
        add_columns([(0, cols_of(axis, forwarded, step)) for axis in (0, 1)], ROWS, CHUNK, True)

    def own_piece(step, forwarded):
        add_columns([(0, piece_of(2 + 2 * axis + forwarded, piece_at(axis, step))) for axis in (0, 1)], ROWS, PIECE, True)

    def far_columns(step, forwarded):
        add_columns([(Y_ROWS, cols_of(0, forwarded, step)), (X_ROWS, cols_of(1, forwarded, step))], HALF, CHUNK, False)

    def far_piece(step, forwarded):
        add_columns([(Y_ROWS, piece_of(2 + forwarded, piece_at(0, step))),
                     (X_ROWS, piece_of(4 + forwarded, piece_at(1, step)))], HALF, PIECE, False)

    set_rows(0, 0, ROWS)

    @pl.loop(0, N_CHUNK)
    def _(c):
        @pl.when(c == N_CHUNK // 2)
        def _():
            for copy in pair_copies():
                copy.wait_recv()
        add_columns([(0, rows_of(0, 2 * c)), (0, rows_of(0, 2 * c + 1))], ROWS, CHUNK, True)

    @pl.loop(0, N_PIECE // 2)
    def _(step):
        receive(step)

        @pl.loop(0, 2)
        def _(forwarded):
            @pl.when(forwarded == 1)
            def _():
                receive_forwarded(step)
            own_piece(step, forwarded)

    set_rows(2 * ROWS, X_ROWS, HALF)
    set_rows(4 * ROWS + HALF, Y_ROWS, HALF)

    @pl.loop(0, N_CHUNK + 2)
    def _(c):
        step = c // 2

        @pl.when(c == N_CHUNK)
        def _():
            receive(N_PIECE // 2)
            receive(N_PIECE // 2 + 1)

        @pl.when(c == N_CHUNK + 1)
        def _():
            receive_forwarded(N_PIECE // 2)
            receive_forwarded(N_PIECE // 2 + 1)

        far_columns(step, lax.rem(c, 2))

    @pl.loop(N_CHUNK // 2, N_CHUNK)
    def _(half):
        @pl.when(half == N_CHUNK - 1)
        def _():
            @pl.loop(N_PIECE - 2, N_PIECE)
            def _(step):
                receive(step)

                @pl.loop(0, 2)
                def _(forwarded):
                    @pl.when(forwarded == 1)
                    def _():
                        receive_forwarded(step)
                    far_piece(step, forwarded)

            for axis in (0, 1):
                back_copy(axis).start()

        @pl.loop(0, 2)
        def _(forwarded):
            own_columns(half, forwarded)

    for axis in (0, 1):
        back_copy(axis).wait_recv()
    out_ref[...] = acc[pl.ds(0, ROWS), :] + back[...]

    for copy in pair_copies():
        copy.wait_send()
    for axis in (0, 1):
        back_copy(axis).wait_send()
        for piece in range(N_PIECE):
            for copy in link_copies(axis, piece) + fwd_copies(axis, piece):
                copy.wait_send()


def solution(mesh):
    row_spec = P(('tasks', 'group'), None)
    dma = pltpu.SemaphoreType.DMA

    def local_fn(x_loc, v_loc, lengthscale, outscale):
        return pl.pallas_call(
            local_kernel,
            out_shape=pltpu.VMEM((ROWS, RHS), jnp.float32),
            in_specs=[pl.BlockSpec(memory_space=pl.ANY), pl.BlockSpec(memory_space=pl.ANY),
                      pl.BlockSpec(memory_space=pltpu.SMEM), pl.BlockSpec(memory_space=pltpu.SMEM)],
            out_specs=pl.BlockSpec(memory_space=pltpu.VMEM),
            scratch_shapes=[
                pltpu.VMEM((6 * ROWS, FEAT), jnp.bfloat16),
                pltpu.VMEM((6 * ROWS, RHS), jnp.bfloat16),
                pltpu.VMEM((2 * ROWS, FEAT), jnp.bfloat16),
                pltpu.VMEM((2 * ROWS, 128), jnp.float32),
                pltpu.VMEM((2 * ROWS, RHS), jnp.float32),
                pltpu.VMEM((ROWS, RHS), jnp.float32),
                dma((2,)), dma((2,)), dma((2,)),
                dma((2, 2, N_PIECE)), dma((2, 2, N_PIECE)),
                dma((2, 2, N_PIECE)), dma((2, 2, N_PIECE)),
                dma((2,)), dma((2,)),
            ],
            compiler_params=pltpu.CompilerParams(collective_id=0, has_side_effects=True, vmem_limit_bytes=60 * 2 ** 20),
        )(x_loc, v_loc, lengthscale, outscale)

    return jax.shard_map(local_fn, mesh=mesh, in_specs=(row_spec, row_spec, P(None), P(None)), out_specs=row_spec, check_vma=False)
```

```python
import functools

import jax
import jax.numpy as jnp
from jax import lax
from jax.experimental import pallas as pl
from jax.experimental.pallas import tpu as pltpu
from jax.sharding import PartitionSpec as P

ROWS = 2048
HALF = ROWS // 2
CHUNK = 512
PIECE = 256
TAIL = ((6, 1536, 256), (7, 1792, 128), (8, 1920, 128))
N_CHUNK = ROWS // CHUNK
TRANSFERS = tuple((i, i * PIECE, PIECE) for i in range(6)) + TAIL
SUB = 256
FEAT = 512
RHS = 128
LOG2E = 1.4426950408889634
OWN, PAIR = 0, 1
X_ROWS, Y_ROWS = ROWS, ROWS + HALF


def local_kernel(x_hbm, v_hbm, ell_ref, scale_ref, out_ref,
                 x_all, v_all, lhs, norm_lhs, acc, back,
                 load_sem, pair_send, pair_recv, link_send, link_recv,
                 fwd_send, fwd_recv, back_send, back_recv):
    me = lax.axis_index('group')
    core = lax.rem(me, 2)
    chip_x = lax.rem(me // 2, 2)
    chip_y = me // 4
    pair = me + 1 - 2 * core
    neighbour = (me + 2 - 4 * chip_x, me + 4 - 8 * chip_y)

    load_x = pltpu.make_async_copy(x_hbm, x_all.at[pl.ds(0, ROWS)], load_sem.at[0])
    load_v = pltpu.make_async_copy(v_hbm, v_all.at[pl.ds(0, ROWS)], load_sem.at[1])
    load_x.start()
    load_v.start()

    barrier = pltpu.get_barrier_semaphore()
    for peer in (pair,) + neighbour:
        pl.semaphore_signal(barrier, inc=1, device_id={'group': peer}, device_id_type=pl.DeviceIdType.MESH)
    pl.semaphore_wait(barrier, 3)

    def remote(src, dst, send, recv, peer):
        return pltpu.make_async_remote_copy(src_ref=src, dst_ref=dst, send_sem=send, recv_sem=recv,
                                            device_id={'group': peer}, device_id_type=pl.DeviceIdType.MESH)

    def rows_of(block, chunk):
        return pl.ds(pl.multiple_of(block * ROWS + chunk * CHUNK, CHUNK), CHUNK)

    def part_of(block, axis, start, width):
        return pl.ds(pl.multiple_of(block * ROWS + lax.rem(start + HALF * axis, ROWS), width), width)

    def pair_copies():
        return (remote(x_all.at[pl.ds(0, ROWS)], x_all.at[pl.ds(PAIR * ROWS, ROWS)], pair_send.at[0], pair_recv.at[0], pair),
                remote(v_all.at[pl.ds(0, ROWS)], v_all.at[pl.ds(PAIR * ROWS, ROWS)], pair_send.at[1], pair_recv.at[1], pair))

    def link_copies(axis, index, start, width):
        src, dst = part_of(OWN, axis, start, width), part_of(2 + 2 * axis, axis, start, width)
        return (remote(x_hbm.at[src], x_all.at[dst], link_send.at[0, axis, index], link_recv.at[0, axis, index], neighbour[axis]),
                remote(v_hbm.at[src], v_all.at[dst], link_send.at[1, axis, index], link_recv.at[1, axis, index], neighbour[axis]))

    def fwd_copies(axis, index, start, width):
        src, dst = part_of(2 + 2 * axis, axis, start, width), part_of(3 + 2 * axis, axis, start, width)
        return (remote(x_all.at[src], x_all.at[dst], fwd_send.at[0, axis, index], fwd_recv.at[0, axis, index], pair),
                remote(v_all.at[src], v_all.at[dst], fwd_send.at[1, axis, index], fwd_recv.at[1, axis, index], pair))

    def back_copy(axis):
        return remote(acc.at[pl.ds(ROWS + axis * HALF, HALF)], back.at[pl.ds(axis * HALF, HALF)],
                      back_send.at[axis], back_recv.at[axis], neighbour[axis])

    for index, start, width in TRANSFERS:
        for axis in (0, 1):
            for copy in link_copies(axis, index, start, width):
                copy.start()
    load_x.wait()
    load_v.wait()
    for copy in pair_copies():
        copy.start()

    ell = jnp.full((8, 128), ell_ref[0], jnp.float32)
    rate = (-LOG2E / (2.0 * (ell * ell)))[0, 0]
    scale = scale_ref[0]

    def set_rows(source, target, count):
        @pl.loop(0, count // CHUNK)
        def _(part):
            rows = x_all[pl.ds(pl.multiple_of(source + part * CHUNK, CHUNK), CHUNK), :]
            at = pl.ds(pl.multiple_of(target + part * CHUNK, CHUNK), CHUNK)
            lhs[at, :] = rows * jnp.bfloat16(-2)
            wide = rows.astype(jnp.float32)
            norm_lhs[at, :] = jnp.broadcast_to(jnp.sum(wide * wide, axis=1, keepdims=True), (CHUNK, 128))
            acc[at, :] = jnp.zeros((CHUNK, RHS), jnp.float32)

    def add_columns(items, row_count, width, same_rows):
        work = []
        for row_start, cols in items:
            x_col = x_all[cols, :]
            wide = x_col.astype(jnp.float32)
            norm_col = jnp.broadcast_to(jnp.sum(wide * wide, axis=1, keepdims=True), (width, 128)).T[0:1, :]
            for i in range(row_count // SUB):
                rows = pl.ds(pl.multiple_of(row_start + i * SUB, SUB), SUB)
                gram = lax.dot_general(lhs[rows, :], x_col, (((1,), (1,)), ((), ())), preferred_element_type=jnp.float32)
                work.append((rows, cols, norm_col, gram))
        def part_sum(rows, cols, norm_col, gram):
            norm_row = jnp.concatenate([norm_lhs[rows, :]] * (width // 128), axis=1)
            dist = jnp.maximum((norm_row + norm_col) + gram, 0.0)
            kern = (scale * jnp.exp2(dist * rate)).astype(jnp.bfloat16)
            return jnp.dot(kern, v_all[cols, :], preferred_element_type=jnp.float32)
        per_item = row_count // SUB
        if same_rows:
            for i in range(per_item):
                acc[work[i][0], :] += part_sum(*work[i]) + part_sum(*work[per_item + i])
        else:
            for one in work:
                acc[one[0], :] += part_sum(*one)

    def receive(index, start, width):
        for axis in (0, 1):
            for copy in link_copies(axis, index, start, width):
                copy.wait_recv()
            for copy in fwd_copies(axis, index, start, width):
                copy.start()

    def receive_forwarded(index, start, width):
        for axis in (0, 1):
            for copy in fwd_copies(axis, index, start, width):
                copy.wait_recv()

    def own_columns(start, width, forwarded):
        add_columns([(0, part_of(2 + 2 * axis + forwarded, axis, start, width)) for axis in (0, 1)], ROWS, width, True)

    def far_columns(start, width, forwarded):
        add_columns([(Y_ROWS, part_of(2 + forwarded, 0, start, width)),
                     (X_ROWS, part_of(4 + forwarded, 1, start, width))], HALF, width, False)

    set_rows(0, 0, ROWS)

    @pl.loop(0, N_CHUNK)
    def _(c):
        @pl.when(c == N_CHUNK // 2)
        def _():
            for copy in pair_copies():
                copy.wait_recv()
        add_columns([(0, rows_of(0, 2 * c)), (0, rows_of(0, 2 * c + 1))], ROWS, CHUNK, True)

    @pl.loop(0, HALF // PIECE)
    def _(index):
        receive(index, index * PIECE, PIECE)

        @pl.loop(0, 2)
        def _(forwarded):
            @pl.when(forwarded == 1)
            def _():
                receive_forwarded(index, index * PIECE, PIECE)
            own_columns(index * PIECE, PIECE, forwarded)

    set_rows(2 * ROWS, X_ROWS, HALF)
    set_rows(4 * ROWS + HALF, Y_ROWS, HALF)

    @pl.loop(0, 6)
    def _(c):
        @pl.when(c == 4)
        def _():
            receive(4, HALF, PIECE)
            receive(5, HALF + PIECE, PIECE)

        @pl.when(c == 5)
        def _():
            receive_forwarded(4, HALF, PIECE)
            receive_forwarded(5, HALF + PIECE, PIECE)

        far_columns(c // 2 * CHUNK, CHUNK, lax.rem(c, 2))

    @pl.loop(0, 4)
    def _(c):
        @pl.when(c == 1)
        def _():
            for index, start, width in TAIL:
                receive(index, start, width)

                @pl.loop(0, 2)
                def _(forwarded):
                    @pl.when(forwarded == 1)
                    def _():
                        receive_forwarded(index, start, width)
                    far_columns(start, width, forwarded)

            for axis in (0, 1):
                back_copy(axis).start()

        own_columns(HALF + c // 2 * CHUNK, CHUNK, lax.rem(c, 2))

    for axis in (0, 1):
        back_copy(axis).wait_recv()
    out_ref[...] = acc[pl.ds(0, ROWS), :] + back[...]

    for copy in pair_copies():
        copy.wait_send()
    for axis in (0, 1):
        back_copy(axis).wait_send()
        for transfer in TRANSFERS:
            for copy in link_copies(axis, *transfer) + fwd_copies(axis, *transfer):
                copy.wait_send()


def solution(mesh):
    row_spec = P(('tasks', 'group'), None)
    dma = pltpu.SemaphoreType.DMA

    def local_fn(x_loc, v_loc, lengthscale, outscale):
        return pl.pallas_call(
            local_kernel,
            out_shape=pltpu.VMEM((ROWS, RHS), jnp.float32),
            in_specs=[pl.BlockSpec(memory_space=pl.ANY), pl.BlockSpec(memory_space=pl.ANY),
                      pl.BlockSpec(memory_space=pltpu.SMEM), pl.BlockSpec(memory_space=pltpu.SMEM)],
            out_specs=pl.BlockSpec(memory_space=pltpu.VMEM),
            scratch_shapes=[
                pltpu.VMEM((6 * ROWS, FEAT), jnp.bfloat16),
                pltpu.VMEM((6 * ROWS, RHS), jnp.bfloat16),
                pltpu.VMEM((2 * ROWS, FEAT), jnp.bfloat16),
                pltpu.VMEM((2 * ROWS, 128), jnp.float32),
                pltpu.VMEM((2 * ROWS, RHS), jnp.float32),
                pltpu.VMEM((ROWS, RHS), jnp.float32),
                dma((2,)), dma((2,)), dma((2,)),
                dma((2, 2, len(TRANSFERS))), dma((2, 2, len(TRANSFERS))),
                dma((2, 2, len(TRANSFERS))), dma((2, 2, len(TRANSFERS))),
                dma((2,)), dma((2,)),
            ],
            compiler_params=pltpu.CompilerParams(collective_id=0, has_side_effects=True, vmem_limit_bytes=60 * 2 ** 20),
        )(x_loc, v_loc, lengthscale, outscale)

    return jax.shard_map(local_fn, mesh=mesh, in_specs=(row_spec, row_spec, P(None), P(None)), out_specs=row_spec, check_vma=False)
```

```python
import functools

import jax
import jax.numpy as jnp
from jax import lax
from jax.experimental import pallas as pl
from jax.experimental.pallas import tpu as pltpu
from jax.sharding import PartitionSpec as P

ROWS = 2048
HALF = ROWS // 2
CHUNK = 512
PIECE = 256
TAIL = ((6, 1536, 256), (7, 1792, 128), (8, 1920, 128))
N_CHUNK = ROWS // CHUNK
TRANSFERS = tuple((i, i * PIECE, PIECE) for i in range(6)) + TAIL
SUB = 256
GROUPS = ((0, 256), (256, 768))
FEAT = 512
RHS = 128
LOG2E = 1.4426950408889634
OWN, PAIR = 0, 1
X_ROWS, Y_ROWS = ROWS, ROWS + HALF


def local_kernel(x_hbm, v_hbm, ell_ref, scale_ref, out_ref,
                 x_all, v_all, lhs, norm_lhs, norm_cols, acc, back,
                 load_sem, pair_send, pair_recv, link_send, link_recv,
                 fwd_send, fwd_recv, back_send, back_recv):
    me = lax.axis_index('group')
    core = lax.rem(me, 2)
    chip_x = lax.rem(me // 2, 2)
    chip_y = me // 4
    pair = me + 1 - 2 * core
    neighbour = (me + 2 - 4 * chip_x, me + 4 - 8 * chip_y)

    load_x = pltpu.make_async_copy(x_hbm, x_all.at[pl.ds(0, ROWS)], load_sem.at[0])
    load_v = pltpu.make_async_copy(v_hbm, v_all.at[pl.ds(0, ROWS)], load_sem.at[1])
    load_x.start()
    load_v.start()

    barrier = pltpu.get_barrier_semaphore()
    for peer in (pair,) + neighbour:
        pl.semaphore_signal(barrier, inc=1, device_id={'group': peer}, device_id_type=pl.DeviceIdType.MESH)
    pl.semaphore_wait(barrier, 3)

    def remote(src, dst, send, recv, peer):
        return pltpu.make_async_remote_copy(src_ref=src, dst_ref=dst, send_sem=send, recv_sem=recv,
                                            device_id={'group': peer}, device_id_type=pl.DeviceIdType.MESH)

    def rows_of(block, chunk):
        return pl.ds(pl.multiple_of(block * ROWS + chunk * CHUNK, CHUNK), CHUNK)

    def part_of(block, axis, start, width):
        return pl.ds(pl.multiple_of(block * ROWS + lax.rem(start + HALF * axis, ROWS), width), width)

    def pair_copies():
        return (remote(x_all.at[pl.ds(0, ROWS)], x_all.at[pl.ds(PAIR * ROWS, ROWS)], pair_send.at[0], pair_recv.at[0], pair),
                remote(v_all.at[pl.ds(0, ROWS)], v_all.at[pl.ds(PAIR * ROWS, ROWS)], pair_send.at[1], pair_recv.at[1], pair))

    def link_copies(axis, index, start, width):
        src, dst = part_of(OWN, axis, start, width), part_of(2 + 2 * axis, axis, start, width)
        return (remote(x_hbm.at[src], x_all.at[dst], link_send.at[0, axis, index], link_recv.at[0, axis, index], neighbour[axis]),
                remote(v_hbm.at[src], v_all.at[dst], link_send.at[1, axis, index], link_recv.at[1, axis, index], neighbour[axis]))

    def fwd_copies(axis, index, start, width):
        src, dst = part_of(2 + 2 * axis, axis, start, width), part_of(3 + 2 * axis, axis, start, width)
        return (remote(x_all.at[src], x_all.at[dst], fwd_send.at[0, axis, index], fwd_recv.at[0, axis, index], pair),
                remote(v_all.at[src], v_all.at[dst], fwd_send.at[1, axis, index], fwd_recv.at[1, axis, index], pair))

    def back_copy(axis, group):
        first, count = GROUPS[group]
        return remote(acc.at[pl.ds(ROWS + axis * HALF + first, count)], back.at[pl.ds(axis * HALF + first, count)],
                      back_send.at[axis, group], back_recv.at[axis, group], neighbour[axis])

    for index, start, width in TRANSFERS:
        for axis in (0, 1):
            for copy in link_copies(axis, index, start, width):
                copy.start()
    load_x.wait()
    load_v.wait()
    for copy in pair_copies():
        copy.start()

    ell = jnp.full((8, 128), ell_ref[0], jnp.float32)
    rate = (-LOG2E / (2.0 * (ell * ell)))[0, 0]
    scale = scale_ref[0]

    def set_rows(source, target, count):
        @pl.loop(0, count // CHUNK)
        def _(part):
            rows = x_all[pl.ds(pl.multiple_of(source + part * CHUNK, CHUNK), CHUNK), :]
            at = pl.ds(pl.multiple_of(target + part * CHUNK, CHUNK), CHUNK)
            lhs[at, :] = rows * jnp.bfloat16(-2)
            wide = rows.astype(jnp.float32)
            norm_lhs[at, :] = jnp.broadcast_to(jnp.sum(wide * wide, axis=1, keepdims=True), (CHUNK, 128))
            acc[at, :] = jnp.zeros((CHUNK, RHS), jnp.float32)

    def add_columns(items, row_count, width, same_rows, known_norms, keep_norms=True):
        work = []
        for row_start, cols in items:
            x_col = x_all[cols, :]
            if known_norms:
                norm_col = norm_cols[0:1, cols]
            else:
                wide = x_col.astype(jnp.float32)
                norm_col = jnp.broadcast_to(jnp.sum(wide * wide, axis=1, keepdims=True), (width, 128)).T[0:1, :]
                if keep_norms:
                    norm_cols[0:1, cols] = norm_col
            for i in range(row_count // SUB):
                rows = pl.ds(pl.multiple_of(row_start + i * SUB, SUB), SUB)
                gram = lax.dot_general(lhs[rows, :], x_col, (((1,), (1,)), ((), ())), preferred_element_type=jnp.float32)
                work.append((rows, cols, norm_col, gram))
        def part_sum(rows, cols, norm_col, gram):
            norm_row = jnp.concatenate([norm_lhs[rows, :]] * (width // 128), axis=1)
            dist = jnp.maximum((norm_row + norm_col) + gram, 0.0)
            kern = (scale * jnp.exp2(dist * rate)).astype(jnp.bfloat16)
            return jnp.dot(kern, v_all[cols, :], preferred_element_type=jnp.float32)
        per_item = row_count // SUB
        if same_rows:
            for i in range(per_item):
                acc[work[i][0], :] += part_sum(*work[i]) + part_sum(*work[per_item + i])
        else:
            for one in work:
                acc[one[0], :] += part_sum(*one)

    def receive(index, start, width):
        for axis in (0, 1):
            for copy in link_copies(axis, index, start, width):
                copy.wait_recv()
            for copy in fwd_copies(axis, index, start, width):
                copy.start()

    def receive_forwarded(index, start, width):
        for axis in (0, 1):
            for copy in fwd_copies(axis, index, start, width):
                copy.wait_recv()

    def own_columns(start, width, forwarded, known_norms):
        add_columns([(0, part_of(2 + 2 * axis + forwarded, axis, start, width)) for axis in (0, 1)], ROWS, width, True, known_norms)

    def far_columns(start, width, forwarded, known_norms, first=0, count=HALF):
        add_columns([(Y_ROWS + first, part_of(2 + forwarded, 0, start, width)),
                     (X_ROWS + first, part_of(4 + forwarded, 1, start, width))], count, width, False, known_norms)

    set_rows(0, 0, ROWS)

    @pl.loop(0, N_CHUNK)
    def _(c):
        @pl.when(c == N_CHUNK // 2)
        def _():
            for copy in pair_copies():
                copy.wait_recv()
        add_columns([(0, rows_of(0, 2 * c)), (0, rows_of(0, 2 * c + 1))], ROWS, CHUNK, True, False, False)

    @pl.loop(0, HALF // PIECE)
    def _(index):
        receive(index, index * PIECE, PIECE)

        @pl.loop(0, 2)
        def _(forwarded):
            @pl.when(forwarded == 1)
            def _():
                receive_forwarded(index, index * PIECE, PIECE)
            own_columns(index * PIECE, PIECE, forwarded, False)

    set_rows(2 * ROWS, X_ROWS, HALF)
    set_rows(4 * ROWS + HALF, Y_ROWS, HALF)

    @pl.loop(0, 4)
    def _(c):
        far_columns(c // 2 * CHUNK, CHUNK, lax.rem(c, 2), True)

    receive(4, HALF, PIECE)
    receive(5, HALF + PIECE, PIECE)

    @pl.loop(0, 2)
    def _(forwarded):
        @pl.when(forwarded == 1)
        def _():
            receive_forwarded(4, HALF, PIECE)
            receive_forwarded(5, HALF + PIECE, PIECE)
        far_columns(HALF, CHUNK, forwarded, False)

    @pl.loop(0, 4)
    def _(c):
        @pl.when(c == 1)
        def _():
            for index, start, width in TAIL[:-1]:
                receive(index, start, width)

                @pl.loop(0, 2)
                def _(forwarded):
                    @pl.when(forwarded == 1)
                    def _():
                        receive_forwarded(index, start, width)
                    far_columns(start, width, forwarded, False)

            index, start, width = TAIL[-1]
            receive(index, start, width)
            far_columns(start, width, 0, False)
            receive_forwarded(index, start, width)
            for group, (first, count) in enumerate(GROUPS):
                far_columns(start, width, 1, group > 0, first, count)
                for axis in (0, 1):
                    back_copy(axis, group).start()

        own_columns(HALF + c // 2 * CHUNK, CHUNK, lax.rem(c, 2), True)

    for group, (first, count) in enumerate(GROUPS):
        for axis in (0, 1):
            back_copy(axis, group).wait_recv()
            rows = pl.ds(axis * HALF + first, count)
            out_ref[rows, :] = acc[rows, :] + back[rows, :]

    for copy in pair_copies():
        copy.wait_send()
    for axis in (0, 1):
        for group in range(len(GROUPS)):
            back_copy(axis, group).wait_send()
        for transfer in TRANSFERS:
            for copy in link_copies(axis, *transfer) + fwd_copies(axis, *transfer):
                copy.wait_send()


def solution(mesh):
    row_spec = P(('tasks', 'group'), None)
    dma = pltpu.SemaphoreType.DMA

    def local_fn(x_loc, v_loc, lengthscale, outscale):
        return pl.pallas_call(
            local_kernel,
            out_shape=pltpu.VMEM((ROWS, RHS), jnp.float32),
            in_specs=[pl.BlockSpec(memory_space=pl.ANY), pl.BlockSpec(memory_space=pl.ANY),
                      pl.BlockSpec(memory_space=pltpu.SMEM), pl.BlockSpec(memory_space=pltpu.SMEM)],
            out_specs=pl.BlockSpec(memory_space=pltpu.VMEM),
            scratch_shapes=[
                pltpu.VMEM((6 * ROWS, FEAT), jnp.bfloat16),
                pltpu.VMEM((6 * ROWS, RHS), jnp.bfloat16),
                pltpu.VMEM((2 * ROWS, FEAT), jnp.bfloat16),
                pltpu.VMEM((2 * ROWS, 128), jnp.float32),
                pltpu.VMEM((8, 6 * ROWS), jnp.float32),
                pltpu.VMEM((2 * ROWS, RHS), jnp.float32),
                pltpu.VMEM((ROWS, RHS), jnp.float32),
                dma((2,)), dma((2,)), dma((2,)),
                dma((2, 2, len(TRANSFERS))), dma((2, 2, len(TRANSFERS))),
                dma((2, 2, len(TRANSFERS))), dma((2, 2, len(TRANSFERS))),
                dma((2, len(GROUPS))), dma((2, len(GROUPS))),
            ],
            compiler_params=pltpu.CompilerParams(collective_id=0, has_side_effects=True, vmem_limit_bytes=60 * 2 ** 20),
        )(x_loc, v_loc, lengthscale, outscale)

    return jax.shard_map(local_fn, mesh=mesh, in_specs=(row_spec, row_spec, P(None), P(None)), out_specs=row_spec, check_vma=False)
```

```python
import functools

import jax
import jax.numpy as jnp
from jax import lax
from jax.experimental import pallas as pl
from jax.experimental.pallas import tpu as pltpu
from jax.sharding import PartitionSpec as P

ROWS = 2048
HALF = ROWS // 2
CHUNK = 512
PIECE = 256
TAIL = ((3, 1536, 256), (4, 1792, 256))
N_CHUNK = ROWS // CHUNK
TRANSFERS = ((0, 0, CHUNK), (1, CHUNK, CHUNK), (2, HALF, CHUNK)) + TAIL
SUB = 256
GROUPS = ((0, 256), (256, 768))
FEAT = 512
RHS = 128
LOG2E = 1.4426950408889634
OWN, PAIR = 0, 1
X_ROWS, Y_ROWS = ROWS, ROWS + HALF


def local_kernel(x_hbm, v_hbm, ell_ref, scale_ref, out_ref,
                 x_all, v_all, lhs, norm_lhs, norm_cols, acc, back,
                 load_sem, pair_send, pair_recv, link_send, link_recv,
                 fwd_send, fwd_recv, back_send, back_recv):
    me = lax.axis_index('group')
    core = lax.rem(me, 2)
    chip_x = lax.rem(me // 2, 2)
    chip_y = me // 4
    pair = me + 1 - 2 * core
    neighbour = (me + 2 - 4 * chip_x, me + 4 - 8 * chip_y)

    load_x = pltpu.make_async_copy(x_hbm, x_all.at[pl.ds(0, ROWS)], load_sem.at[0])
    load_v = pltpu.make_async_copy(v_hbm, v_all.at[pl.ds(0, ROWS)], load_sem.at[1])
    load_x.start()
    load_v.start()

    barrier = pltpu.get_barrier_semaphore()
    for peer in (pair,) + neighbour:
        pl.semaphore_signal(barrier, inc=1, device_id={'group': peer}, device_id_type=pl.DeviceIdType.MESH)
    pl.semaphore_wait(barrier, 3)

    def remote(src, dst, send, recv, peer):
        return pltpu.make_async_remote_copy(src_ref=src, dst_ref=dst, send_sem=send, recv_sem=recv,
                                            device_id={'group': peer}, device_id_type=pl.DeviceIdType.MESH)

    def rows_of(block, chunk):
        return pl.ds(pl.multiple_of(block * ROWS + chunk * CHUNK, CHUNK), CHUNK)

    def part_of(block, axis, start, width):
        return pl.ds(pl.multiple_of(block * ROWS + lax.rem(start + HALF * axis, ROWS), width), width)

    def pair_copies():
        return (remote(x_all.at[pl.ds(0, ROWS)], x_all.at[pl.ds(PAIR * ROWS, ROWS)], pair_send.at[0], pair_recv.at[0], pair),
                remote(v_all.at[pl.ds(0, ROWS)], v_all.at[pl.ds(PAIR * ROWS, ROWS)], pair_send.at[1], pair_recv.at[1], pair))

    def link_copies(axis, index, start, width):
        src, dst = part_of(OWN, axis, start, width), part_of(2 + 2 * axis, axis, start, width)
        return (remote(x_hbm.at[src], x_all.at[dst], link_send.at[0, axis, index], link_recv.at[0, axis, index], neighbour[axis]),
                remote(v_hbm.at[src], v_all.at[dst], link_send.at[1, axis, index], link_recv.at[1, axis, index], neighbour[axis]))

    def fwd_copies(axis, index, start, width):
        src, dst = part_of(2 + 2 * axis, axis, start, width), part_of(3 + 2 * axis, axis, start, width)
        return (remote(x_all.at[src], x_all.at[dst], fwd_send.at[0, axis, index], fwd_recv.at[0, axis, index], pair),
                remote(v_all.at[src], v_all.at[dst], fwd_send.at[1, axis, index], fwd_recv.at[1, axis, index], pair))

    def back_copy(axis, group):
        first, count = GROUPS[group]
        return remote(acc.at[pl.ds(ROWS + axis * HALF + first, count)], back.at[pl.ds(axis * HALF + first, count)],
                      back_send.at[axis, group], back_recv.at[axis, group], neighbour[axis])

    for index, start, width in TRANSFERS:
        for axis in (0, 1):
            for copy in link_copies(axis, index, start, width):
                copy.start()
    load_x.wait()
    load_v.wait()
    for copy in pair_copies():
        copy.start()

    ell = jnp.full((8, 128), ell_ref[0], jnp.float32)
    rate = (-LOG2E / (2.0 * (ell * ell)))[0, 0]
    scale = scale_ref[0]

    def set_rows(source, target, count):
        @pl.loop(0, count // CHUNK)
        def _(part):
            rows = x_all[pl.ds(pl.multiple_of(source + part * CHUNK, CHUNK), CHUNK), :]
            at = pl.ds(pl.multiple_of(target + part * CHUNK, CHUNK), CHUNK)
            lhs[at, :] = rows * jnp.bfloat16(-2)
            wide = rows.astype(jnp.float32)
            norm_lhs[at, :] = jnp.broadcast_to(jnp.sum(wide * wide, axis=1, keepdims=True), (CHUNK, 128))
            acc[at, :] = jnp.zeros((CHUNK, RHS), jnp.float32)

    def add_columns(items, row_count, width, same_rows, known_norms, keep_norms=True):
        work = []
        for row_start, cols in items:
            x_col = x_all[cols, :]
            if known_norms:
                norm_col = norm_cols[0:1, cols]
            else:
                wide = x_col.astype(jnp.float32)
                norm_col = jnp.broadcast_to(jnp.sum(wide * wide, axis=1, keepdims=True), (width, 128)).T[0:1, :]
                if keep_norms:
                    norm_cols[0:1, cols] = norm_col
            for i in range(row_count // SUB):
                rows = pl.ds(pl.multiple_of(row_start + i * SUB, SUB), SUB)
                gram = lax.dot_general(lhs[rows, :], x_col, (((1,), (1,)), ((), ())), preferred_element_type=jnp.float32)
                work.append((rows, cols, norm_col, gram))
        def part_sum(rows, cols, norm_col, gram):
            norm_row = jnp.concatenate([norm_lhs[rows, :]] * (width // 128), axis=1)
            dist = jnp.maximum((norm_row + norm_col) + gram, 0.0)
            kern = (scale * jnp.exp2(dist * rate)).astype(jnp.bfloat16)
            return jnp.dot(kern, v_all[cols, :], preferred_element_type=jnp.float32)
        per_item = row_count // SUB
        if same_rows:
            for i in range(per_item):
                acc[work[i][0], :] += part_sum(*work[i]) + part_sum(*work[per_item + i])
        else:
            for one in work:
                acc[one[0], :] += part_sum(*one)

    def receive(index, start, width):
        for axis in (0, 1):
            for copy in link_copies(axis, index, start, width):
                copy.wait_recv()
            for copy in fwd_copies(axis, index, start, width):
                copy.start()

    def receive_forwarded(index, start, width):
        for axis in (0, 1):
            for copy in fwd_copies(axis, index, start, width):
                copy.wait_recv()

    def own_columns(start, width, forwarded, known_norms):
        add_columns([(0, part_of(2 + 2 * axis + forwarded, axis, start, width)) for axis in (0, 1)], ROWS, width, True, known_norms)

    def far_columns(start, width, forwarded, known_norms, first=0, count=HALF):
        add_columns([(Y_ROWS + first, part_of(2 + forwarded, 0, start, width)),
                     (X_ROWS + first, part_of(4 + forwarded, 1, start, width))], count, width, False, known_norms)

    set_rows(0, 0, ROWS)

    @pl.loop(0, N_CHUNK)
    def _(c):
        @pl.when(c == N_CHUNK // 2)
        def _():
            for copy in pair_copies():
                copy.wait_recv()
        add_columns([(0, rows_of(0, 2 * c)), (0, rows_of(0, 2 * c + 1))], ROWS, CHUNK, True, False, False)

    @pl.loop(0, HALF // CHUNK)
    def _(index):
        receive(index, index * CHUNK, CHUNK)

        @pl.loop(0, 2)
        def _(forwarded):
            @pl.when(forwarded == 1)
            def _():
                receive_forwarded(index, index * CHUNK, CHUNK)
            own_columns(index * CHUNK, CHUNK, forwarded, False)

    set_rows(2 * ROWS, X_ROWS, HALF)
    set_rows(4 * ROWS + HALF, Y_ROWS, HALF)

    @pl.loop(0, 4)
    def _(c):
        far_columns(c // 2 * CHUNK, CHUNK, lax.rem(c, 2), True)

    receive(2, HALF, CHUNK)

    @pl.loop(0, 2)
    def _(forwarded):
        @pl.when(forwarded == 1)
        def _():
            receive_forwarded(2, HALF, CHUNK)
        far_columns(HALF, CHUNK, forwarded, False)

    @pl.loop(0, 4)
    def _(c):
        @pl.when(c == 1)
        def _():
            for index, start, width in TAIL[:-1]:
                receive(index, start, width)

                @pl.loop(0, 2)
                def _(forwarded):
                    @pl.when(forwarded == 1)
                    def _():
                        receive_forwarded(index, start, width)
                    far_columns(start, width, forwarded, False)

            index, start, width = TAIL[-1]
            receive(index, start, width)
            for group, (first, count) in enumerate(GROUPS):
                far_columns(start, width, 0, group > 0, first, count)
                if group == 0:
                    receive_forwarded(index, start, width)
                far_columns(start, width, 1, group > 0, first, count)
                for axis in (0, 1):
                    back_copy(axis, group).start()

        own_columns(HALF + c // 2 * CHUNK, CHUNK, lax.rem(c, 2), True)

    for group, (first, count) in enumerate(GROUPS):
        for axis in (0, 1):
            back_copy(axis, group).wait_recv()
            rows = pl.ds(axis * HALF + first, count)
            out_ref[rows, :] = acc[rows, :] + back[rows, :]

    for copy in pair_copies():
        copy.wait_send()
    for axis in (0, 1):
        for group in range(len(GROUPS)):
            back_copy(axis, group).wait_send()
        for transfer in TRANSFERS:
            for copy in link_copies(axis, *transfer) + fwd_copies(axis, *transfer):
                copy.wait_send()


def solution(mesh):
    row_spec = P(('tasks', 'group'), None)
    dma = pltpu.SemaphoreType.DMA

    def local_fn(x_loc, v_loc, lengthscale, outscale):
        return pl.pallas_call(
            local_kernel,
            out_shape=pltpu.VMEM((ROWS, RHS), jnp.float32),
            in_specs=[pl.BlockSpec(memory_space=pl.ANY), pl.BlockSpec(memory_space=pl.ANY),
                      pl.BlockSpec(memory_space=pltpu.SMEM), pl.BlockSpec(memory_space=pltpu.SMEM)],
            out_specs=pl.BlockSpec(memory_space=pltpu.VMEM),
            scratch_shapes=[
                pltpu.VMEM((6 * ROWS, FEAT), jnp.bfloat16),
                pltpu.VMEM((6 * ROWS, RHS), jnp.bfloat16),
                pltpu.VMEM((2 * ROWS, FEAT), jnp.bfloat16),
                pltpu.VMEM((2 * ROWS, 128), jnp.float32),
                pltpu.VMEM((8, 6 * ROWS), jnp.float32),
                pltpu.VMEM((2 * ROWS, RHS), jnp.float32),
                pltpu.VMEM((ROWS, RHS), jnp.float32),
                dma((2,)), dma((2,)), dma((2,)),
                dma((2, 2, len(TRANSFERS))), dma((2, 2, len(TRANSFERS))),
                dma((2, 2, len(TRANSFERS))), dma((2, 2, len(TRANSFERS))),
                dma((2, len(GROUPS))), dma((2, len(GROUPS))),
            ],
            compiler_params=pltpu.CompilerParams(collective_id=0, has_side_effects=True, vmem_limit_bytes=60 * 2 ** 20),
        )(x_loc, v_loc, lengthscale, outscale)

    return jax.shard_map(local_fn, mesh=mesh, in_specs=(row_spec, row_spec, P(None), P(None)), out_specs=row_spec, check_vma=False)
```

```python
import functools

import jax
import jax.numpy as jnp
from jax import lax
from jax.experimental import pallas as pl
from jax.experimental.pallas import tpu as pltpu
from jax.sharding import PartitionSpec as P

ROWS = 2048
HALF = ROWS // 2
CHUNK = 512
PIECE = 256
TAIL = ((3, 1536, 256), (4, 1792, 256))
N_CHUNK = ROWS // CHUNK
TRANSFERS = ((0, 0, CHUNK), (1, CHUNK, CHUNK), (2, HALF, CHUNK)) + TAIL
SUB = 256
GROUPS = ((0, 256), (256, 768))
FEAT = 512
RHS = 128
LOG2E = 1.4426950408889634
OWN, PAIR = 0, 1
X_ROWS, Y_ROWS = ROWS, ROWS + HALF


def local_kernel(x_hbm, v_hbm, ell_ref, scale_ref, out_ref,
                 x_all, v_all, lhs, norm_lhs, norm_cols, acc, back,
                 load_sem, pair_send, pair_recv, link_send, link_recv,
                 fwd_send, fwd_recv, back_send, back_recv):
    me = lax.axis_index('group')
    core = lax.rem(me, 2)
    chip_x = lax.rem(me // 2, 2)
    chip_y = me // 4
    pair = me + 1 - 2 * core
    neighbour = (me + 2 - 4 * chip_x, me + 4 - 8 * chip_y)

    load_x = pltpu.make_async_copy(x_hbm, x_all.at[pl.ds(0, ROWS)], load_sem.at[0])
    load_v = pltpu.make_async_copy(v_hbm, v_all.at[pl.ds(0, ROWS)], load_sem.at[1])
    load_x.start()
    load_v.start()

    barrier = pltpu.get_barrier_semaphore()
    for peer in (pair,) + neighbour:
        pl.semaphore_signal(barrier, inc=1, device_id={'group': peer}, device_id_type=pl.DeviceIdType.MESH)
    pl.semaphore_wait(barrier, 3)

    def remote(src, dst, send, recv, peer):
        return pltpu.make_async_remote_copy(src_ref=src, dst_ref=dst, send_sem=send, recv_sem=recv,
                                            device_id={'group': peer}, device_id_type=pl.DeviceIdType.MESH)

    def rows_of(block, chunk):
        return pl.ds(pl.multiple_of(block * ROWS + chunk * CHUNK, CHUNK), CHUNK)

    def part_of(block, axis, start, width):
        return pl.ds(pl.multiple_of(block * ROWS + lax.rem(start + HALF * axis, ROWS), width), width)

    def pair_copies():
        return (remote(x_all.at[pl.ds(0, ROWS)], x_all.at[pl.ds(PAIR * ROWS, ROWS)], pair_send.at[0], pair_recv.at[0], pair),
                remote(v_all.at[pl.ds(0, ROWS)], v_all.at[pl.ds(PAIR * ROWS, ROWS)], pair_send.at[1], pair_recv.at[1], pair))

    def both(index, axis, src_block, dst_block, start, width, x_src, v_src, send, recv, peer):
        copies = (remote(x_src.at[part_of(src_block, axis, start, width)], x_all.at[part_of(dst_block, axis, start, width)],
                         send.at[0, axis, index], recv.at[0, axis, index], peer),)
        if isinstance(index, int) and index == TAIL[-1][0]:
            return copies
        rows = CHUNK
        return copies + (remote(v_src.at[part_of(src_block, axis, start, rows)], v_all.at[part_of(dst_block, axis, start, rows)],
                                send.at[1, axis, index], recv.at[1, axis, index], peer),)

    def link_copies(axis, index, start, width):
        return both(index, axis, OWN, 2 + 2 * axis, start, width, x_hbm, v_hbm, link_send, link_recv, neighbour[axis])

    def fwd_copies(axis, index, start, width):
        return both(index, axis, 2 + 2 * axis, 3 + 2 * axis, start, width, x_all, v_all, fwd_send, fwd_recv, pair)

    def back_copy(axis, group):
        first, count = GROUPS[group]
        return remote(acc.at[pl.ds(ROWS + axis * HALF + first, count)], back.at[pl.ds(axis * HALF + first, count)],
                      back_send.at[axis, group], back_recv.at[axis, group], neighbour[axis])

    for index, start, width in TRANSFERS:
        for axis in (0, 1):
            for copy in link_copies(axis, index, start, width):
                copy.start()
    load_x.wait()
    load_v.wait()
    for copy in pair_copies():
        copy.start()

    ell = jnp.full((8, 128), ell_ref[0], jnp.float32)
    rate = (-LOG2E / (2.0 * (ell * ell)))[0, 0]
    scale = scale_ref[0]

    def set_rows(source, target, count):
        @pl.loop(0, count // CHUNK)
        def _(part):
            rows = x_all[pl.ds(pl.multiple_of(source + part * CHUNK, CHUNK), CHUNK), :]
            at = pl.ds(pl.multiple_of(target + part * CHUNK, CHUNK), CHUNK)
            lhs[at, :] = rows * jnp.bfloat16(-2)
            wide = rows.astype(jnp.float32)
            norm_lhs[at, :] = jnp.broadcast_to(jnp.sum(wide * wide, axis=1, keepdims=True), (CHUNK, 128))
            acc[at, :] = jnp.zeros((CHUNK, RHS), jnp.float32)

    def add_columns(items, row_count, width, same_rows, known_norms, keep_norms=True):
        work = []
        for row_start, cols in items:
            x_col = x_all[cols, :]
            if known_norms:
                norm_col = norm_cols[0:1, cols]
            else:
                wide = x_col.astype(jnp.float32)
                norm_col = jnp.broadcast_to(jnp.sum(wide * wide, axis=1, keepdims=True), (width, 128)).T[0:1, :]
                if keep_norms:
                    norm_cols[0:1, cols] = norm_col
            for i in range(row_count // SUB):
                rows = pl.ds(pl.multiple_of(row_start + i * SUB, SUB), SUB)
                gram = lax.dot_general(lhs[rows, :], x_col, (((1,), (1,)), ((), ())), preferred_element_type=jnp.float32)
                work.append((rows, cols, norm_col, gram))
        def part_sum(rows, cols, norm_col, gram):
            norm_row = jnp.concatenate([norm_lhs[rows, :]] * (width // 128), axis=1)
            dist = jnp.maximum((norm_row + norm_col) + gram, 0.0)
            kern = (scale * jnp.exp2(dist * rate)).astype(jnp.bfloat16)
            return jnp.dot(kern, v_all[cols, :], preferred_element_type=jnp.float32)
        per_item = row_count // SUB
        if same_rows:
            for i in range(per_item):
                acc[work[i][0], :] += part_sum(*work[i]) + part_sum(*work[per_item + i])
        else:
            for one in work:
                acc[one[0], :] += part_sum(*one)

    def receive(index, start, width):
        for axis in (0, 1):
            for copy in link_copies(axis, index, start, width):
                copy.wait_recv()
            for copy in fwd_copies(axis, index, start, width):
                copy.start()

    def receive_forwarded(index, start, width):
        for axis in (0, 1):
            for copy in fwd_copies(axis, index, start, width):
                copy.wait_recv()

    def own_columns(start, width, forwarded, known_norms):
        add_columns([(0, part_of(2 + 2 * axis + forwarded, axis, start, width)) for axis in (0, 1)], ROWS, width, True, known_norms)

    def far_columns(start, width, forwarded, known_norms, first=0, count=HALF):
        add_columns([(Y_ROWS + first, part_of(2 + forwarded, 0, start, width)),
                     (X_ROWS + first, part_of(4 + forwarded, 1, start, width))], count, width, False, known_norms)

    set_rows(0, 0, ROWS)

    @pl.loop(0, N_CHUNK)
    def _(c):
        @pl.when(c == N_CHUNK // 2)
        def _():
            for copy in pair_copies():
                copy.wait_recv()
        add_columns([(0, rows_of(0, 2 * c)), (0, rows_of(0, 2 * c + 1))], ROWS, CHUNK, True, False, False)

    @pl.loop(0, HALF // CHUNK)
    def _(index):
        receive(index, index * CHUNK, CHUNK)

        @pl.loop(0, 2)
        def _(forwarded):
            @pl.when(forwarded == 1)
            def _():
                receive_forwarded(index, index * CHUNK, CHUNK)
            own_columns(index * CHUNK, CHUNK, forwarded, False)

    set_rows(2 * ROWS, X_ROWS, HALF)
    set_rows(4 * ROWS + HALF, Y_ROWS, HALF)

    @pl.loop(0, 4)
    def _(c):
        far_columns(c // 2 * CHUNK, CHUNK, lax.rem(c, 2), True)

    receive(2, HALF, CHUNK)

    @pl.loop(0, 2)
    def _(forwarded):
        @pl.when(forwarded == 1)
        def _():
            receive_forwarded(2, HALF, CHUNK)
        far_columns(HALF, CHUNK, forwarded, False)

    @pl.loop(0, 4)
    def _(c):
        @pl.when(c == 1)
        def _():
            for index, start, width in TAIL[:-1]:
                receive(index, start, width)

                @pl.loop(0, 2)
                def _(forwarded):
                    @pl.when(forwarded == 1)
                    def _():
                        receive_forwarded(index, start, width)
                    far_columns(start, width, forwarded, False)

            index, start, width = TAIL[-1]
            receive(index, start, width)
            for group, (first, count) in enumerate(GROUPS):
                far_columns(start, width, 0, group > 0, first, count)
                if group == 0:
                    receive_forwarded(index, start, width)
                far_columns(start, width, 1, group > 0, first, count)
                for axis in (0, 1):
                    back_copy(axis, group).start()

        own_columns(HALF + c // 2 * CHUNK, CHUNK, lax.rem(c, 2), True)

    for group, (first, count) in enumerate(GROUPS):
        for axis in (0, 1):
            back_copy(axis, group).wait_recv()
            rows = pl.ds(axis * HALF + first, count)
            out_ref[rows, :] = acc[rows, :] + back[rows, :]

    for copy in pair_copies():
        copy.wait_send()
    for axis in (0, 1):
        for group in range(len(GROUPS)):
            back_copy(axis, group).wait_send()
        for transfer in TRANSFERS:
            for copy in link_copies(axis, *transfer) + fwd_copies(axis, *transfer):
                copy.wait_send()


def solution(mesh):
    row_spec = P(('tasks', 'group'), None)
    dma = pltpu.SemaphoreType.DMA

    def local_fn(x_loc, v_loc, lengthscale, outscale):
        return pl.pallas_call(
            local_kernel,
            out_shape=pltpu.VMEM((ROWS, RHS), jnp.float32),
            in_specs=[pl.BlockSpec(memory_space=pl.ANY), pl.BlockSpec(memory_space=pl.ANY),
                      pl.BlockSpec(memory_space=pltpu.SMEM), pl.BlockSpec(memory_space=pltpu.SMEM)],
            out_specs=pl.BlockSpec(memory_space=pltpu.VMEM),
            scratch_shapes=[
                pltpu.VMEM((6 * ROWS, FEAT), jnp.bfloat16),
                pltpu.VMEM((6 * ROWS, RHS), jnp.bfloat16),
                pltpu.VMEM((2 * ROWS, FEAT), jnp.bfloat16),
                pltpu.VMEM((2 * ROWS, 128), jnp.float32),
                pltpu.VMEM((8, 6 * ROWS), jnp.float32),
                pltpu.VMEM((2 * ROWS, RHS), jnp.float32),
                pltpu.VMEM((ROWS, RHS), jnp.float32),
                dma((2,)), dma((2,)), dma((2,)),
                dma((2, 2, len(TRANSFERS))), dma((2, 2, len(TRANSFERS))),
                dma((2, 2, len(TRANSFERS))), dma((2, 2, len(TRANSFERS))),
                dma((2, len(GROUPS))), dma((2, len(GROUPS))),
            ],
            compiler_params=pltpu.CompilerParams(collective_id=0, has_side_effects=True, vmem_limit_bytes=60 * 2 ** 20),
        )(x_loc, v_loc, lengthscale, outscale)

    return jax.shard_map(local_fn, mesh=mesh, in_specs=(row_spec, row_spec, P(None), P(None)), out_specs=row_spec, check_vma=False)
```

```python
import functools

import jax
import jax.numpy as jnp
from jax import lax
from jax.experimental import pallas as pl
from jax.experimental.pallas import tpu as pltpu
from jax.sharding import PartitionSpec as P

ROWS = 2048
HALF = ROWS // 2
CHUNK = 512
PIECE = 256
TAIL = ((3, 1536, 256), (4, 1792, 256))
N_CHUNK = ROWS // CHUNK
TRANSFERS = ((0, 0, CHUNK), (1, CHUNK, CHUNK), (2, HALF, CHUNK)) + TAIL
SUB = 256
GROUPS = ((0, 256), (256, 768))
FEAT = 512
RHS = 128
LOG2E = 1.4426950408889634
OWN, PAIR = 0, 1
X_ROWS, Y_ROWS = ROWS, ROWS + HALF


def local_kernel(x_hbm, v_hbm, ell_ref, scale_ref, out_ref,
                 x_all, v_all, lhs, norm_lhs, norm_cols, acc, back,
                 load_sem, pair_send, pair_recv, link_send, link_recv,
                 fwd_send, fwd_recv, back_send, back_recv):
    me = lax.axis_index('group')
    core = lax.rem(me, 2)
    chip_x = lax.rem(me // 2, 2)
    chip_y = me // 4
    pair = me + 1 - 2 * core
    neighbour = (me + 2 - 4 * chip_x, me + 4 - 8 * chip_y)

    load_x = pltpu.make_async_copy(x_hbm, x_all.at[pl.ds(0, ROWS)], load_sem.at[0])
    load_v = pltpu.make_async_copy(v_hbm, v_all.at[pl.ds(0, ROWS)], load_sem.at[1])
    load_x.start()
    load_v.start()

    barrier = pltpu.get_barrier_semaphore()
    for peer in (pair,) + neighbour:
        pl.semaphore_signal(barrier, inc=1, device_id={'group': peer}, device_id_type=pl.DeviceIdType.MESH)
    pl.semaphore_wait(barrier, 3)

    def remote(src, dst, send, recv, peer):
        return pltpu.make_async_remote_copy(src_ref=src, dst_ref=dst, send_sem=send, recv_sem=recv,
                                            device_id={'group': peer}, device_id_type=pl.DeviceIdType.MESH)

    def rows_of(block, chunk):
        return pl.ds(pl.multiple_of(block * ROWS + chunk * CHUNK, CHUNK), CHUNK)

    def part_of(block, axis, start, width):
        return pl.ds(pl.multiple_of(block * ROWS + lax.rem(start + HALF * axis, ROWS), width), width)

    def pair_copies():
        return (remote(x_all.at[pl.ds(0, ROWS)], x_all.at[pl.ds(PAIR * ROWS, ROWS)], pair_send.at[0], pair_recv.at[0], pair),
                remote(v_all.at[pl.ds(0, ROWS)], v_all.at[pl.ds(PAIR * ROWS, ROWS)], pair_send.at[1], pair_recv.at[1], pair))

    def both(index, axis, src_block, dst_block, start, width, x_src, v_src, send, recv, peer):
        copies = (remote(x_src.at[part_of(src_block, axis, start, width)], x_all.at[part_of(dst_block, axis, start, width)],
                         send.at[0, axis, index], recv.at[0, axis, index], peer),)
        if isinstance(index, int) and index >= TAIL[0][0]:
            return copies
        rows = HALF if isinstance(index, int) and index == TAIL[0][0] - 1 else CHUNK
        return copies + (remote(v_src.at[part_of(src_block, axis, start, rows)], v_all.at[part_of(dst_block, axis, start, rows)],
                                send.at[1, axis, index], recv.at[1, axis, index], peer),)

    def link_copies(axis, index, start, width):
        return both(index, axis, OWN, 2 + 2 * axis, start, width, x_hbm, v_hbm, link_send, link_recv, neighbour[axis])

    def fwd_copies(axis, index, start, width):
        return both(index, axis, 2 + 2 * axis, 3 + 2 * axis, start, width, x_all, v_all, fwd_send, fwd_recv, pair)

    def back_copy(axis, group):
        first, count = GROUPS[group]
        return remote(acc.at[pl.ds(ROWS + axis * HALF + first, count)], back.at[pl.ds(axis * HALF + first, count)],
                      back_send.at[axis, group], back_recv.at[axis, group], neighbour[axis])

    for index, start, width in TRANSFERS:
        for axis in (0, 1):
            for copy in link_copies(axis, index, start, width):
                copy.start()
    load_x.wait()
    load_v.wait()
    for copy in pair_copies():
        copy.start()

    ell = jnp.full((8, 128), ell_ref[0], jnp.float32)
    rate = (-LOG2E / (2.0 * (ell * ell)))[0, 0]
    scale = scale_ref[0]

    def set_rows(source, target, count):
        @pl.loop(0, count // CHUNK)
        def _(part):
            rows = x_all[pl.ds(pl.multiple_of(source + part * CHUNK, CHUNK), CHUNK), :]
            at = pl.ds(pl.multiple_of(target + part * CHUNK, CHUNK), CHUNK)
            lhs[at, :] = rows * jnp.bfloat16(-2)
            wide = rows.astype(jnp.float32)
            norm_lhs[at, :] = jnp.broadcast_to(jnp.sum(wide * wide, axis=1, keepdims=True), (CHUNK, 128))
            acc[at, :] = jnp.zeros((CHUNK, RHS), jnp.float32)

    def add_columns(items, row_count, width, same_rows, known_norms, keep_norms=True):
        work = []
        for row_start, cols in items:
            x_col = x_all[cols, :]
            if known_norms:
                norm_col = norm_cols[0:1, cols]
            else:
                wide = x_col.astype(jnp.float32)
                norm_col = jnp.broadcast_to(jnp.sum(wide * wide, axis=1, keepdims=True), (width, 128)).T[0:1, :]
                if keep_norms:
                    norm_cols[0:1, cols] = norm_col
            for i in range(row_count // SUB):
                rows = pl.ds(pl.multiple_of(row_start + i * SUB, SUB), SUB)
                gram = lax.dot_general(lhs[rows, :], x_col, (((1,), (1,)), ((), ())), preferred_element_type=jnp.float32)
                work.append((rows, cols, norm_col, gram))
        def part_sum(rows, cols, norm_col, gram):
            norm_row = jnp.concatenate([norm_lhs[rows, :]] * (width // 128), axis=1)
            dist = jnp.maximum((norm_row + norm_col) + gram, 0.0)
            kern = (scale * jnp.exp2(dist * rate)).astype(jnp.bfloat16)
            return jnp.dot(kern, v_all[cols, :], preferred_element_type=jnp.float32)
        per_item = row_count // SUB
        if same_rows:
            for i in range(per_item):
                acc[work[i][0], :] += part_sum(*work[i]) + part_sum(*work[per_item + i])
        else:
            for one in work:
                acc[one[0], :] += part_sum(*one)

    def receive(index, start, width):
        for axis in (0, 1):
            for copy in link_copies(axis, index, start, width):
                copy.wait_recv()
            for copy in fwd_copies(axis, index, start, width):
                copy.start()

    def receive_forwarded(index, start, width):
        for axis in (0, 1):
            for copy in fwd_copies(axis, index, start, width):
                copy.wait_recv()

    def own_columns(start, width, forwarded, known_norms):
        add_columns([(0, part_of(2 + 2 * axis + forwarded, axis, start, width)) for axis in (0, 1)], ROWS, width, True, known_norms)

    def far_columns(start, width, forwarded, known_norms, first=0, count=HALF):
        add_columns([(Y_ROWS + first, part_of(2 + forwarded, 0, start, width)),
                     (X_ROWS + first, part_of(4 + forwarded, 1, start, width))], count, width, False, known_norms)

    set_rows(0, 0, ROWS)

    @pl.loop(0, N_CHUNK)
    def _(c):
        @pl.when(c == N_CHUNK // 2)
        def _():
            for copy in pair_copies():
                copy.wait_recv()
        add_columns([(0, rows_of(0, 2 * c)), (0, rows_of(0, 2 * c + 1))], ROWS, CHUNK, True, False, False)

    @pl.loop(0, HALF // CHUNK)
    def _(index):
        receive(index, index * CHUNK, CHUNK)

        @pl.loop(0, 2)
        def _(forwarded):
            @pl.when(forwarded == 1)
            def _():
                receive_forwarded(index, index * CHUNK, CHUNK)
            own_columns(index * CHUNK, CHUNK, forwarded, False)

    set_rows(2 * ROWS, X_ROWS, HALF)
    set_rows(4 * ROWS + HALF, Y_ROWS, HALF)

    @pl.loop(0, 4)
    def _(c):
        far_columns(c // 2 * CHUNK, CHUNK, lax.rem(c, 2), True)

    receive(2, HALF, CHUNK)

    @pl.loop(0, 2)
    def _(forwarded):
        @pl.when(forwarded == 1)
        def _():
            receive_forwarded(2, HALF, CHUNK)
        far_columns(HALF, CHUNK, forwarded, False)

    @pl.loop(0, 4)
    def _(c):
        @pl.when(c == 1)
        def _():
            for index, start, width in TAIL[:-1]:
                receive(index, start, width)

                @pl.loop(0, 2)
                def _(forwarded):
                    @pl.when(forwarded == 1)
                    def _():
                        receive_forwarded(index, start, width)
                    far_columns(start, width, forwarded, False)

            index, start, width = TAIL[-1]
            receive(index, start, width)
            for group, (first, count) in enumerate(GROUPS):
                far_columns(start, width, 0, group > 0, first, count)
                if group == 0:
                    receive_forwarded(index, start, width)
                far_columns(start, width, 1, group > 0, first, count)
                for axis in (0, 1):
                    back_copy(axis, group).start()

        own_columns(HALF + c // 2 * CHUNK, CHUNK, lax.rem(c, 2), True)

    for group, (first, count) in enumerate(GROUPS):
        for axis in (0, 1):
            back_copy(axis, group).wait_recv()
            rows = pl.ds(axis * HALF + first, count)
            out_ref[rows, :] = acc[rows, :] + back[rows, :]

    for copy in pair_copies():
        copy.wait_send()
    for axis in (0, 1):
        for group in range(len(GROUPS)):
            back_copy(axis, group).wait_send()
        for transfer in TRANSFERS:
            for copy in link_copies(axis, *transfer) + fwd_copies(axis, *transfer):
                copy.wait_send()


def solution(mesh):
    row_spec = P(('tasks', 'group'), None)
    dma = pltpu.SemaphoreType.DMA

    def local_fn(x_loc, v_loc, lengthscale, outscale):
        return pl.pallas_call(
            local_kernel,
            out_shape=pltpu.VMEM((ROWS, RHS), jnp.float32),
            in_specs=[pl.BlockSpec(memory_space=pl.ANY), pl.BlockSpec(memory_space=pl.ANY),
                      pl.BlockSpec(memory_space=pltpu.SMEM), pl.BlockSpec(memory_space=pltpu.SMEM)],
            out_specs=pl.BlockSpec(memory_space=pltpu.VMEM),
            scratch_shapes=[
                pltpu.VMEM((6 * ROWS, FEAT), jnp.bfloat16),
                pltpu.VMEM((6 * ROWS, RHS), jnp.bfloat16),
                pltpu.VMEM((2 * ROWS, FEAT), jnp.bfloat16),
                pltpu.VMEM((2 * ROWS, 128), jnp.float32),
                pltpu.VMEM((8, 6 * ROWS), jnp.float32),
                pltpu.VMEM((2 * ROWS, RHS), jnp.float32),
                pltpu.VMEM((ROWS, RHS), jnp.float32),
                dma((2,)), dma((2,)), dma((2,)),
                dma((2, 2, len(TRANSFERS))), dma((2, 2, len(TRANSFERS))),
                dma((2, 2, len(TRANSFERS))), dma((2, 2, len(TRANSFERS))),
                dma((2, len(GROUPS))), dma((2, len(GROUPS))),
            ],
            compiler_params=pltpu.CompilerParams(collective_id=0, has_side_effects=True, vmem_limit_bytes=60 * 2 ** 20),
        )(x_loc, v_loc, lengthscale, outscale)

    return jax.shard_map(local_fn, mesh=mesh, in_specs=(row_spec, row_spec, P(None), P(None)), out_specs=row_spec, check_vma=False)
```
